128 devices in a mesh: up: 16 (over y_lo, x, core), dn: 8 (over y_hi, z).
Axes of the slice: x: 4, y: 4 (y_hi: 2, y_lo: 2; y = y_hi * 2 + y_lo), z: 4, core: 2. Of those that a mesh axis runs over, the one named last changes fastest.
Arguments:
- start_vector: bfloat16 [13312, 13312], P('up', 'dn'), may hold values from -6 to 6
- hop_tiles: bfloat16 [104, 5, 128, 128], replicated, may hold values from -0.5 to 0.5
- tile_columns: int32 [104, 5], replicated, may hold values from 0 to 103, as said below
- tile_signs: int32 [104, 5], replicated, may hold values from 0 to 1
- occupation: int32 [16, 13312], replicated, may hold values from 0 to 1, as said below
Outputs:
- next_vector: bfloat16 [13312, 13312], P('up', 'dn')
- alphas: float32 [2], replicated
- betas: float32 [2], replicated
The draws below stay inside these ranges and needn't reach their ends.
Inputs may be any that keep to these rules, and one draw needn't show every extreme that they name: Each row of tile_columns names 5 different tile columns. Every column of occupation holds exactly 8 ones.
All inputs are finite; a program needn't handle non-finite values.
Results may differ from the reference program's by a relative error of at most 0.0065.
Values may be sent and summed in bfloat16 or wider, within the bound.
A program may use at most 192 MiB of HBM per device.

```python
import jax
import jax.numpy as jnp
from jax import lax

DETS = 13312
SITES = 16
TILE = 128
TILE_K = 5
STEPS = 2
TILES = 104


def draw_tile_columns(key, part):
    scores = jax.random.randint(key, (TILES, TILES), 0, 1 << 20) * TILES + jnp.arange(TILES, dtype=jnp.int32)[None, :]
    order = jnp.argsort(scores, axis=1)
    return order[:, :TILE_K].astype(jnp.int32)


def draw_occupation(key, part):
    scores = jax.random.randint(key, (DETS, SITES), 0, 1 << 20) * SITES + jnp.arange(SITES, dtype=jnp.int32)[None, :]
    ranks = jnp.argsort(jnp.argsort(scores, axis=1), axis=1)
    filled = (ranks < SITES // 2).astype(jnp.int32)
    return filled.T


def with_ends(drawn, key, smallest, high):
    dims = drawn.shape
    index_at = [jax.random.randint(jax.random.fold_in(key, axis), (), 0, dims[axis]) for axis in range(len(dims))]
    drawn = drawn.at[tuple(index_at)].set(smallest)
    longest = dims.index(max(dims))
    index_at[longest] = (index_at[longest] + 1) % dims[longest]
    return drawn.at[tuple(index_at)].set(high)


def block_scale(key, dims, shards, smallest, high):
    level = 1.0
    for dim, blocks in shards:
        draws = jax.random.uniform(jax.random.fold_in(jax.random.fold_in(key, 6), dim), (blocks,), jnp.float32, smallest / len(shards), high / len(shards))
        level = level * jnp.repeat(jnp.exp(draws), dims[dim] // blocks).reshape((-1,) + (1,) * (len(dims) - 1 - dim))
    return level


def bell_draw(rng, shape, spread, most, pieces=(), held_as=jnp.bfloat16):
    loudness = block_scale(rng, shape, pieces, -0.22, 0.18) if pieces else 1.0
    entries = jax.random.normal(rng, shape, jnp.float32) * spread * loudness
    return jnp.minimum(jnp.maximum(entries, -most), most).astype(held_as)


def setup_inputs(seed: int = 0) -> dict:
    seeds = jax.random.split(jax.random.key(seed), 6)
    start_vector = bell_draw(seeds[0], (DETS, DETS), 1.0, 6.0, ((0, 16), (1, 8)))
    hop_tiles = bell_draw(seeds[1], (TILES, TILE_K, TILE, TILE), TILE ** -0.5, 0.5)
    tile_columns = draw_tile_columns(jax.random.fold_in(seeds[5], 71), 0)
    tile_signs = with_ends(jax.random.randint(seeds[3], (TILES, TILE_K), 0, 2), jax.random.fold_in(seeds[3], 1), 0, 1).astype(jnp.int32)
    occupation = draw_occupation(jax.random.fold_in(seeds[5], 71), 0)
    return {"start_vector": start_vector, "hop_tiles": hop_tiles, "tile_columns": tile_columns, "tile_signs": tile_signs, "occupation": occupation}


coupling = 4.0

def hop_last(matrix, signed_wide, tile_columns):

    def one_block(part):
        cube = part.reshape(part.shape[0], TILES, TILE)
        picked = cube[:, tile_columns].astype(jnp.float32)
        result = jnp.einsum('ikab,mikb->mia', signed_wide, picked, precision=lax.Precision.HIGHEST)
        return result.reshape(part.shape)
    blocks = matrix.reshape(-1, 512, matrix.shape[1])
    return lax.map(one_block, blocks).reshape(matrix.shape)

def reference(start_vector, hop_tiles, tile_columns, tile_signs, occupation):
    signed = hop_tiles * (1 - 2 * tile_signs).astype(jnp.bfloat16)[:, :, None, None]
    signed_wide = signed.astype(jnp.float32)
    occupied = occupation.astype(jnp.bfloat16)
    diagonal = coupling * jnp.dot(occupied.T, occupied, preferred_element_type=jnp.float32)
    vector = start_vector.astype(jnp.float32)
    total = jnp.sum(vector * vector)
    vector = vector / jnp.maximum(jnp.sqrt(total), 1.0)
    previous = jnp.zeros_like(vector)
    beta_value = jnp.float32(0.0)
    alpha_list = []
    beta_list = []
    for iteration in range(STEPS):
        rounded = vector.astype(jnp.bfloat16)
        hopped_up = hop_last(rounded.T, signed_wide, tile_columns).T.astype(jnp.bfloat16)
        hopped_down = hop_last(rounded, signed_wide, tile_columns).astype(jnp.bfloat16)
        work = hopped_up.astype(jnp.float32) + hopped_down.astype(jnp.float32) + diagonal * vector - beta_value * previous
        intersect = jnp.sum(work * vector)
        work = work - intersect * vector
        residual = jnp.sum(work * work)
        beta_value = jnp.sqrt(jnp.maximum(residual, 1.0))
        previous = vector
        vector = work / beta_value
        alpha_list.append(intersect)
        beta_list.append(beta_value)
    return (vector.astype(jnp.bfloat16), jnp.stack(alpha_list), jnp.stack(beta_list))
```

```python
import functools

import jax
import jax.numpy as jnp
from jax import lax
from jax.experimental import pallas as pl
from jax.experimental.pallas import tpu as pltpu
from jax.sharding import Mesh
from jax.sharding import PartitionSpec as P

STEPS = 2
UP = ("up_0", "up_1", "up_2")
DN = ("dn_0", "dn_1")
UP_DN = ("up_0", "up_1", "up_2", "dn_0", "dn_1")


coupling = 4.0


def split_up(value, dim, peers):
    before, after = (value.shape[:dim], value.shape[dim + 1 :])
    return jnp.moveaxis(value.reshape(*before, peers, -1, *after), dim, 0)


def joined_along(pieces, dim):
    pieces = jnp.moveaxis(pieces, 0, dim)
    shape = pieces.shape
    return pieces.reshape(*shape[:dim], shape[dim] * shape[dim + 1], *shape[dim + 2 :])


def moved_by_axis(pieces, axes, order):
    inside = pieces.shape[1:]
    whole = pieces.reshape(*(lax.axis_size(a) for a in axes), *inside)
    for k in order:
        whole = lax.all_to_all(whole, axes[k], k, k, tiled=True)
    return whole.reshape(-1, *inside)


def exchange_by_chip(value, groups, order, split_dim, concat_dim):
    peers = lax.axis_size(groups[0]) * lax.axis_size(groups[1])
    pieces = split_up(value, split_dim, peers)
    return joined_along(moved_by_axis(pieces, groups, order), concat_dim)


def edges_of(length, count):
    step = length // count
    if step >= 8:
        step -= step % 8
    return [step * k for k in range(1, count)]


def cut_exchange(value, axis, pieces, split_dim, concat_dim):
    blocks = split_up(value, split_dim, lax.axis_size(axis))
    cut = max(range(1, max(2, blocks.ndim - 1)), key=lambda d: blocks.shape[d])
    gathered = []
    for piece in jnp.split(blocks, edges_of(blocks.shape[cut], pieces), axis=cut):
        if piece.size:
            gathered.append(lax.all_to_all(piece, axis, split_axis=0, concat_axis=0, tiled=True))
    return joined_along(jnp.concatenate(gathered, axis=cut), concat_dim)


MESH_ID = pl.DeviceIdType.MESH


def coords(index):
    return (index // 64, lax.rem(index // 16, 4), lax.rem(index // 8, 2), lax.rem(index // 4, 2), lax.rem(index, 4))


def sum_kernel(x_ref, o_ref, src, dst, send_sem, recv_sem):
    count = dst.shape[0]
    me = lax.axis_index(UP_DN)
    barrier = pltpu.get_barrier_semaphore()

    def greet(s, carry):
        pl.semaphore_signal(barrier, inc=1, device_id=coords(lax.rem(me + s, count)), device_id_type=MESH_ID)
        return carry

    lax.fori_loop(1, count, greet, 0)
    src[...] = x_ref[...]
    dst[pl.ds(me, 1)] = x_ref[...].reshape((1, *x_ref.shape))
    pl.semaphore_wait(barrier, count - 1)

    def send(s, carry):
        pltpu.make_async_remote_copy(
            src_ref=src,
            dst_ref=dst.at[me],
            send_sem=send_sem,
            recv_sem=recv_sem,
            device_id=coords(lax.rem(me + s, count)),
            device_id_type=MESH_ID,
        ).start()
        return carry

    lax.fori_loop(1, count, send, 0)
    rest = dst.at[pl.ds(0, count - 1)]
    whole = pltpu.make_async_remote_copy(
        src_ref=rest, dst_ref=rest, send_sem=send_sem, recv_sem=recv_sem, device_id=coords(me), device_id_type=MESH_ID
    )
    whole.wait_recv()
    whole.wait_send()
    o_ref[...] = jnp.sum(dst[...], axis=0)


def summed(values):
    rows = jnp.stack([jnp.broadcast_to(v, (128,)) for v in values] + [jnp.zeros((128,), jnp.float32)] * (8 - len(values)))
    out = pl.pallas_call(
        sum_kernel,
        out_shape=jax.ShapeDtypeStruct((8, 128), jnp.float32),
        in_specs=[pl.BlockSpec(memory_space=pltpu.VMEM)],
        out_specs=pl.BlockSpec(memory_space=pltpu.VMEM),
        scratch_shapes=[
            pltpu.VMEM((8, 128), jnp.float32),
            pltpu.VMEM((128, 8, 128), jnp.float32),
            pltpu.SemaphoreType.DMA,
            pltpu.SemaphoreType.DMA,
        ],
        compiler_params=pltpu.CompilerParams(collective_id=0, has_side_effects=True),
    )(rows)
    return [out[k, 0] for k in range(len(values))]


def hop_lead(matrix, signed, tile_columns):
    layout = matrix.shape
    tile_width = signed.shape[-1]
    cube = matrix.reshape(layout[0] // tile_width, tile_width, -1)
    picked = cube[tile_columns]
    result = jnp.einsum("ikab,ikbm->iam", signed, picked, preferred_element_type=jnp.float32)
    return result.reshape(layout).astype(jnp.bfloat16)


def body(start_vector, hop_tiles, tile_columns, tile_signs, occupation):
    signed = hop_tiles * (1 - 2 * tile_signs).astype(jnp.bfloat16)[:, :, None, None]
    rows_local, cols_local = start_vector.shape
    count_up = lax.axis_size(UP)
    count_down = lax.axis_size(DN)
    row_start = lax.axis_index(UP) * rows_local
    col_start = lax.axis_index(DN) * cols_local
    block_rows, block_cols = start_vector.shape
    occ_rows = lax.dynamic_slice_in_dim(occupation, row_start, block_rows, 1).astype(jnp.bfloat16)
    occ_cols = lax.dynamic_slice_in_dim(occupation, col_start, block_cols, 1).astype(jnp.bfloat16)
    diagonal = coupling * jnp.einsum(
        "sa,sb->ab", occ_rows, occ_cols, preferred_element_type=jnp.float32
    )
    vector = start_vector.astype(jnp.float32)
    (total,) = summed([jnp.sum(vector * vector)])
    vector = vector / jnp.maximum(jnp.sqrt(total), 1.0)
    length = total / jnp.maximum(total, 1.0)
    previous = jnp.zeros_like(vector)
    beta_value = jnp.float32(0.0)
    alpha_list = []
    beta_list = []
    for iteration in range(STEPS):
        rounded = vector.astype(jnp.bfloat16)
        cube = rounded.reshape(block_rows, count_up, block_cols // count_up)
        up_part = lax.all_to_all(cube, UP, split_axis=1, concat_axis=0, tiled=True)
        up_whole = up_part.reshape(up_part.shape[0], up_part.shape[2])
        up_hopped = hop_lead(up_whole, signed, tile_columns).reshape(up_part.shape)
        moved = exchange_by_chip(up_hopped, (("up_0", "up_1"), "up_2"), (1, 0), 0, 1)
        hopped_up = moved.reshape(block_rows, block_cols)
        flipped = rounded.T.reshape(block_cols, count_down, block_rows // count_down)
        part = lax.all_to_all(flipped, DN, split_axis=1, concat_axis=0, tiled=True)
        whole = part.reshape(part.shape[0], part.shape[2])
        hopped = hop_lead(whole, signed, tile_columns).reshape(part.shape)
        returned = cut_exchange(hopped, DN, 2, 0, 1)
        hopped_down = returned.reshape(block_cols, block_rows).T
        work = (
            hopped_up.astype(jnp.float32)
            + hopped_down.astype(jnp.float32)
            + diagonal * vector
            - beta_value * previous
        )
        intersect, square = summed([jnp.sum(work * vector), jnp.sum(work * work)])
        work = work - intersect * vector
        residual = square - 2.0 * intersect * intersect + intersect * intersect * length
        beta_value = jnp.sqrt(jnp.maximum(residual, 1.0))
        length = residual / jnp.maximum(residual, 1.0)
        previous = vector
        vector = work / beta_value
        alpha_list.append(intersect)
        beta_list.append(beta_value)
    final = vector.astype(jnp.bfloat16)
    return (final, jnp.stack(alpha_list), jnp.stack(beta_list))


def solution(mesh):
    torus = Mesh(mesh.devices.reshape(2, 4, 2, 2, 4), ("up_0", "up_1", "up_2", "dn_0", "dn_1"))
    return jax.shard_map(
        body,
        mesh=torus,
        in_specs=(P(UP, DN), P(), P(), P(), P()),
        out_specs=(P(UP, DN), P(), P()),
        check_vma=False,
    )
```
